32 devices in a mesh: dp: 8 (over z, x), mp: 4 (over y, core).
Axes of the slice: x: 2, y: 2, z: 4, core: 2. Of those that a mesh axis runs over, the one named last changes fastest.
Arguments:
- teacher_states: bfloat16 [512, 128, 4096], P('dp', None, 'mp'), may hold values from -6 to 6
- teacher_gain: float32 [4096], P('mp'), may hold values from 0.25 to 1.75
- teacher_proj: bfloat16 [4096, 1024], P('mp'), may hold values from -0.09375 to 0.09375
- teacher_mask: int32 [512, 128], P('dp'), may hold values 0 or 1
- student_states: bfloat16 [1024, 64, 768], P(('dp', 'mp')), may hold values from -6 to 6
- student_gain: float32 [768], replicated, may hold values from 0.25 to 1.75
- student_proj: bfloat16 [768, 1024], replicated, may hold values from -0.21875 to 0.21875
- student_mask: int32 [1024, 64], P(('dp', 'mp')), may hold values 0 or 1
- positive: int32 [1024], P(('dp', 'mp')), may hold values from 0 to 511
Outputs:
- grad_embed: float32 [1024, 1024], P(('dp', 'mp'))
- grad_states: bfloat16 [1024, 64, 768], P(('dp', 'mp'))
The draws below stay inside these ranges and needn't reach their ends.
All inputs are finite; a program needn't handle non-finite values. No bound on the sum of `teacher_mask` or of `student_mask` on one device may be relied on, other than what follows from the above.
Results may differ from the reference program's by a relative error of at most 0.0085.
Values may be sent and summed in bfloat16 or wider, within the bound.
A program may use at most 128 MiB of HBM per device.

```python
import jax
import jax.numpy as jnp
from jax import lax

D = 4096
E = 1024
DS = 768
LEN = 128
QLEN = 64
PASSAGES = 512
QUERIES = 1024


def place_ends(result, rng, least, high):
    longest = result.shape.index(max(result.shape))
    spots = []
    for shift in (0, 1):
        where = [jax.random.randint(jax.random.fold_in(rng, axis), (), 0, length) for axis, length in enumerate(result.shape)]
        where[longest] = (where[longest] + shift) % result.shape[longest]
        spots.append(tuple(where))
    return result.at[spots[0]].set(least).at[spots[1]].set(high)


def block_scale(own_key, shape, cuts, least, top_value):
    def one(dim, shards_of):
        heights = jax.random.uniform(jax.random.fold_in(jax.random.fold_in(own_key, 6), dim), (shards_of,), jnp.float32, least / len(cuts), top_value / len(cuts))
        return jnp.repeat(jnp.exp(heights), shape[dim] // shards_of).reshape((-1,) + (1,) * (len(shape) - dim - 1))

    level = one(*cuts[0])
    for cut in cuts[1:]:
        level = level * one(*cut)
    return level


def normal_values(rng, shape, spread, reach, cuts=(), kind=jnp.bfloat16):
    drawn = spread * jax.random.normal(rng, shape, jnp.float32)
    if cuts:
        drawn = drawn * block_scale(rng, shape, cuts, -0.22, 0.18)
    return jnp.clip(drawn, -reach, reach).astype(kind)


def setup_inputs(seed: int = 0) -> dict:
    streams_of = jax.random.split(jax.random.key(seed), 10)
    teacher_states = normal_values(streams_of[0], (PASSAGES, LEN, D), 1.0, 6.0, ((0, 8), (2, 4)))
    teacher_gain = jnp.clip(1.0 + 0.15 * jax.random.normal(streams_of[1], (D,), jnp.float32), 0.25, 1.75)
    teacher_proj = normal_values(streams_of[2], (D, E), D ** -0.5, 0.09375, ((0, 4),))
    teacher_mask = place_ends((jax.random.randint(streams_of[3], (PASSAGES, LEN), 0, 4) < 3).astype(jnp.int32), jax.random.fold_in(streams_of[3], 1), 0, 1)
    student_states = normal_values(streams_of[4], (QUERIES, QLEN, DS), 1.0, 6.0, ((0, 32),))
    student_gain = jnp.clip(1.0 + 0.15 * jax.random.normal(streams_of[5], (DS,), jnp.float32), 0.25, 1.75)
    student_proj = normal_values(streams_of[6], (DS, E), DS ** -0.5, 0.21875)
    student_mask = place_ends((jax.random.randint(streams_of[7], (QUERIES, QLEN), 0, 4) < 3).astype(jnp.int32), jax.random.fold_in(streams_of[7], 1), 0, 1)
    positive = place_ends(jax.random.randint(streams_of[8], (QUERIES,), 0, PASSAGES), jax.random.fold_in(streams_of[8], 1), 0, PASSAGES - 1).astype(jnp.int32)
    return dict(teacher_states=teacher_states, teacher_gain=teacher_gain, teacher_proj=teacher_proj, teacher_mask=teacher_mask, student_states=student_states, student_gain=student_gain, student_proj=student_proj, student_mask=student_mask, positive=positive)


def pool_block(pair):
    states, live_mask = pair
    values = states.astype(jnp.float32)
    scale = lax.rsqrt(lax.optimization_barrier(jnp.mean(values * values, axis=-1)) + 1e-06)
    live = live_mask.astype(jnp.float32)
    weight = live * scale
    return lax.optimization_barrier(jnp.sum(values * weight[:, :, None], axis=1))

def unit_rows(values):
    return values * lax.rsqrt(lax.optimization_barrier(jnp.mean(values * values, axis=-1, keepdims=True)) + 1e-06) / jnp.sqrt(jnp.float32(values.shape[-1]))

def student_forward(states, gain, proj, live_mask):
    values = states.astype(jnp.float32)
    scale = lax.rsqrt(lax.optimization_barrier(jnp.mean(values * values, axis=-1, keepdims=True)) + 1e-06)
    normed = (values * scale * gain).astype(jnp.bfloat16)
    flat = normed.reshape(-1, normed.shape[-1])
    act = jax.nn.gelu(jnp.dot(flat, proj, preferred_element_type=jnp.float32), approximate=True)
    act = act.reshape(states.shape[0], states.shape[1], -1)
    live = live_mask.astype(jnp.float32)
    pooled = lax.optimization_barrier(jnp.sum(act * live[:, :, None], axis=1))
    return unit_rows(pooled)

def reference(teacher_states, teacher_gain, teacher_proj, teacher_mask, student_states, student_gain, student_proj, student_mask, positive):
    blocks = teacher_states.reshape(-1, 16, LEN, D)
    masks = teacher_mask.reshape(-1, 16, LEN)
    pooled = lax.map(pool_block, (blocks, masks)).reshape(PASSAGES, D)
    tpooled = (pooled * teacher_gain).astype(jnp.bfloat16)
    traw = jnp.dot(tpooled, teacher_proj, preferred_element_type=jnp.float32)
    temb = unit_rows(traw).astype(jnp.bfloat16)
    semb, back = jax.vjp(lambda st: student_forward(st, student_gain, student_proj, student_mask), student_states)
    sround = semb.astype(jnp.bfloat16)
    tpos = temb[positive]
    tlogit = 10.0 * jnp.dot(tpos, temb.T, preferred_element_type=jnp.float32)
    slogit = 20.0 * jnp.dot(sround, temb.T, preferred_element_type=jnp.float32)
    texp = jnp.exp(tlogit)
    sexp = jnp.exp(slogit)
    diff = (sexp / lax.optimization_barrier(jnp.sum(sexp, axis=1, keepdims=True)) - texp / lax.optimization_barrier(jnp.sum(texp, axis=1, keepdims=True))).astype(jnp.bfloat16)
    grad_embed = 20.0 * jnp.dot(diff, temb, preferred_element_type=jnp.float32)
    grad_states = back(grad_embed)[0]
    return (grad_embed, grad_states.astype(jnp.bfloat16))
```

```python
import functools

import jax
import jax.numpy as jnp
from jax import lax
from jax.experimental import pallas as pl
from jax.experimental.pallas import tpu as pltpu
from jax.sharding import PartitionSpec as P

MESH = pl.DeviceIdType.MESH
F32 = jnp.float32
BF16 = jnp.bfloat16
GROUPS = 4
QC = 4
ROOT = 0.7978845608028654
CUBE = 0.044715
NT = (((1,), (1,)), ((), ()))


def spread(live, chunk, tokens):
    queries, length = live.shape
    wide = jnp.concatenate([live] * (tokens // length), axis=1)
    row = lax.broadcasted_iota(jnp.int32, (queries, tokens), 0)
    col = lax.broadcasted_iota(jnp.int32, (queries, tokens), 1)
    return jnp.where(row == chunk * (tokens // length) + col // length, wide, 0.0)


def front(
    dn, n, ts, tmask, tgain, tproj, ss, sgain, sproj, smask,
    temb_out, raw_out, h_out,
    tx, tp, sx, sp, sq, sqr, tpool, pf, pb, pr, te, hbuf,
    sem_tx, sem_in, sq_send, sq_recv, rs_send, rs_recv, ag_send, ag_recv, dp_send, dp_recv, h_sem, out_sem,
):
    passages, length, feats = tx.shape
    width = n * feats
    rows = passages // n
    embed = tp.shape[1]
    chunks = passages // 8
    tokens = QC * smask.shape[1]
    schunks = sx.shape[0] // tokens
    me_d, me_m = lax.axis_index("dp"), lax.axis_index("mp")

    def mp_peer(o):
        return (me_d, lax.rem(me_m + o, n))

    def dp_peer(o):
        return (lax.rem(me_d + o, dn), me_m)

    def load(c):
        part = pl.ds(c * 8, 8)
        return pltpu.make_async_copy(ts.at[part], tx.at[part], sem_tx.at[c])

    others = [
        pltpu.make_async_copy(ss, sx, sem_in.at[0]),
        pltpu.make_async_copy(sproj, sp, sem_in.at[1]),
        pltpu.make_async_copy(tproj, tp, sem_in.at[2]),
    ]
    for c in range(chunks):
        load(c).start()
    for copy in others:
        copy.start()
    barrier = pltpu.get_barrier_semaphore()
    for o in range(1, n):
        pl.semaphore_signal(barrier, inc=1, device_id=mp_peer(o), device_id_type=MESH)
    for o in range(1, dn):
        pl.semaphore_signal(barrier, inc=1, device_id=dp_peer(o), device_id_type=MESH)

    def remote(src, dst, send, recv, peer):
        return pltpu.make_async_remote_copy(
            src_ref=src, dst_ref=dst, send_sem=send, recv_sem=recv, device_id=peer, device_id_type=MESH
        )

    ones = jnp.ones((16, 128), BF16)
    row8 = lax.broadcasted_iota(jnp.int32, (8, length), 0)
    per = chunks // GROUPS
    sq_copies = []
    for g in range(GROUPS):

        def squares(i, carry):
            c = g * per + i
            load(c).wait()
            held = jnp.zeros((8, length), F32)
            for j in range(8):
                total = None
                for k in range(feats // 128):
                    x = tx[c * 8 + j, :, k * 128 : (k + 1) * 128].astype(F32)
                    total = x * x if total is None else total + x * x
                line = lax.dot_general(ones, total.astype(BF16), NT, preferred_element_type=F32)
                held = jnp.where(row8 == j, line[:8], held)
            sq[c] = held
            return carry

        lax.fori_loop(0, per, squares, 0)
        if g == 0:
            pl.semaphore_wait(barrier, n + dn - 2)
        part = pl.ds(g * per, per)
        for o in range(1, n):
            copy = remote(sq.at[part], sqr.at[o, part], sq_send.at[o, g], sq_recv.at[o, g], mp_peer(o))
            copy.start()
            sq_copies.append(copy)

    row16 = lax.rem(lax.broadcasted_iota(jnp.int32, (16, length), 0), 8)
    for g in range(GROUPS):
        for o in range(1, n):
            sq_copies[g * (n - 1) + o - 1].wait_recv()

        def pool(i, carry):
            c = g * per + i
            total = sq[c]
            for o in range(1, n):
                total = total + sqr[o, c]
            part = pl.ds(pl.multiple_of(c * 8, 8), 8)
            weight = tmask[part, :].astype(F32) * lax.rsqrt(total / width + 1e-06)
            high = weight.astype(BF16).astype(F32)
            both = jnp.concatenate([high, weight - high], axis=0)
            left = jnp.concatenate([jnp.where(row16 == j, both, 0.0) for j in range(8)], axis=1).astype(BF16)
            sums = jnp.dot(left, tx[pl.ds(c * 8, 8)].reshape(8 * length, feats), preferred_element_type=F32)
            tpool[part, :] = (sums[:8] + sums[8:]) * tgain[...]
            return carry

        lax.fori_loop(0, per, pool, 0)

    others[2].wait()
    partial = jnp.dot(tpool[...].astype(BF16), tp[...], preferred_element_type=F32)
    for j in range(n):
        block = partial[j * rows : (j + 1) * rows]
        pf[j] = block
        pb[j] = block.astype(BF16)
    rs_copies = []
    for o in range(1, n):
        copy = remote(pb.at[lax.rem(me_m + o, n)], pr.at[o], rs_send.at[o], rs_recv.at[o], mp_peer(o))
        copy.start()
        rs_copies.append(copy)

    live = smask[...].astype(F32)
    raw_out[...] = jnp.zeros_like(raw_out)
    others[0].wait()
    others[1].wait()

    def keep(i):
        part = pl.ds(pl.multiple_of(i * tokens, tokens), tokens)
        return pltpu.make_async_copy(hbuf.at[part], h_out.at[part], h_sem.at[i])

    def student(i, carry):
        part = pl.ds(pl.multiple_of(i * tokens, tokens), tokens)
        x = sx[part, :].astype(F32)
        scale = lax.rsqrt(jnp.mean(x * x, axis=-1, keepdims=True) + 1e-06)
        normed = (x * scale * sgain[...]).astype(BF16)
        picks = spread(live, i, tokens).astype(BF16)
        for k in range(embed // 256):
            cols = slice(k * 256, (k + 1) * 256)
            u = jnp.dot(normed, sp[:, cols], preferred_element_type=F32)
            uu = u * u
            th = jnp.tanh(u * (ROOT + (ROOT * CUBE) * uu))
            half = 0.5 + 0.5 * th
            act = u * half
            slope = half + act * (1.0 - th) * (ROOT + (3.0 * ROOT * CUBE) * uu)
            hbuf[part, cols] = slope.astype(BF16)
            raw_out[:, cols] += jnp.dot(picks, act.astype(BF16), preferred_element_type=F32)
        keep(i).start()
        return carry

    first, second = schunks // 4, schunks // 2
    lax.fori_loop(0, first, student, 0)

    for copy in rs_copies:
        copy.wait_recv()
    summed = pf[me_m]
    for o in range(1, n):
        summed = summed + pr[o].astype(F32)
    unit = summed * lax.rsqrt(jnp.mean(summed * summed, axis=-1, keepdims=True) + 1e-06) * (embed ** -0.5)
    te[me_d, me_m] = unit.astype(BF16)
    ag_copies = []
    for o in range(1, n):
        copy = remote(te.at[me_d, me_m], te.at[me_d, me_m], ag_send.at[o], ag_recv.at[o], mp_peer(o))
        copy.start()
        ag_copies.append(copy)

    lax.fori_loop(first, second, student, 0)

    for copy in ag_copies:
        copy.wait_recv()
    dp_copies = []
    for o in range(1, dn):
        copy = remote(te.at[me_d], te.at[me_d], dp_send.at[o], dp_recv.at[o], dp_peer(o))
        copy.start()
        dp_copies.append(copy)

    lax.fori_loop(second, schunks, student, 0)

    for copy in dp_copies:
        copy.wait_recv()
    out = pltpu.make_async_copy(te, temb_out, out_sem)
    out.start()
    for copy in sq_copies + rs_copies + ag_copies + dp_copies:
        copy.wait_send()
    for i in range(schunks):
        keep(i).wait()
    out.wait()


def back(temb, raw_ref, pos, smask, sgain, sproj, ss, h, embed_out, states_out, grad):
    step = pl.program_id(0)
    tokens = ss.shape[0]

    @pl.when(step == 0)
    def _():
        raw = raw_ref[...]
        width = raw.shape[1]
        scale = lax.rsqrt(jnp.mean(raw * raw, axis=-1, keepdims=True) + 1e-06)
        unit = scale * (width ** -0.5)
        sround = (raw * unit).astype(BF16)
        table = temb[...]
        columns = lax.broadcasted_iota(jnp.int32, (raw.shape[0], table.shape[0]), 1)
        picker = jnp.where(pos[...] == columns, 1.0, 0.0).astype(BF16)
        tpos = jnp.dot(picker, table, preferred_element_type=F32).astype(BF16)
        both = jnp.concatenate([tpos, sround], axis=0)
        logits = lax.dot_general(both, table, NT, preferred_element_type=F32)
        texp = jnp.exp(10.0 * logits[: raw.shape[0]])
        sexp = jnp.exp(20.0 * logits[raw.shape[0] :])
        diff = sexp / jnp.sum(sexp, axis=1, keepdims=True) - texp / jnp.sum(texp, axis=1, keepdims=True)
        ge = 20.0 * jnp.dot(diff.astype(BF16), table, preferred_element_type=F32)
        embed_out[...] = ge
        inner = jnp.mean(raw * ge, axis=-1, keepdims=True)
        grad[...] = unit * (ge - raw * (scale * scale * inner))

    picks = jnp.transpose(spread(smask[...].astype(F32), step, tokens)).astype(BF16)
    wide = jnp.dot(picks, grad[...].astype(BF16), preferred_element_type=F32)
    du = (h[...].astype(F32) * wide).astype(BF16)
    dn = lax.dot_general(du, sproj[...], NT, preferred_element_type=F32)
    gy = dn.astype(BF16).astype(F32) * sgain[...]
    x = ss[...].astype(F32)
    scale = lax.rsqrt(jnp.mean(x * x, axis=-1, keepdims=True) + 1e-06)
    inner = jnp.mean(x * gy, axis=-1, keepdims=True)
    states_out[...] = (scale * gy - x * (scale * scale * scale * inner)).astype(BF16)


def shards(dn, n, ts, tgain, tproj, tmask, ss, sgain, sproj, smask, positive):
    passages, length, feats = ts.shape
    embed = tproj.shape[1]
    queries, qlen, ds = ss.shape
    rows = passages // n
    total = queries * qlen
    tokens = QC * qlen
    schunks = total // tokens
    chunks = passages // 8
    flat = ss.reshape(total, ds)
    gain1 = sgain.reshape(1, ds)
    anyspace = pl.BlockSpec(memory_space=pl.ANY)
    vmem = pl.BlockSpec(memory_space=pltpu.VMEM)
    dma = pltpu.SemaphoreType.DMA
    temb, raw, h = pl.pallas_call(
        functools.partial(front, dn, n),
        out_shape=(
            jax.ShapeDtypeStruct((dn, n, rows, embed), BF16),
            jax.ShapeDtypeStruct((queries, embed), F32),
            jax.ShapeDtypeStruct((total, embed), BF16),
        ),
        in_specs=[anyspace, vmem, vmem, anyspace, anyspace, vmem, anyspace, vmem],
        out_specs=(anyspace, vmem, anyspace),
        scratch_shapes=[
            pltpu.VMEM((passages, length, feats), BF16),
            pltpu.VMEM((feats, embed), BF16),
            pltpu.VMEM((total, ds), BF16),
            pltpu.VMEM((ds, embed), BF16),
            pltpu.VMEM((chunks, 8, length), F32),
            pltpu.VMEM((n, chunks, 8, length), F32),
            pltpu.VMEM((passages, feats), F32),
            pltpu.VMEM((n, rows, embed), F32),
            pltpu.VMEM((n, rows, embed), BF16),
            pltpu.VMEM((n, rows, embed), BF16),
            pltpu.VMEM((dn, n, rows, embed), BF16),
            pltpu.VMEM((total, embed), BF16),
            dma((chunks,)),
            dma((3,)),
            dma((n, GROUPS)),
            dma((n, GROUPS)),
            dma((n,)),
            dma((n,)),
            dma((n,)),
            dma((n,)),
            dma((dn,)),
            dma((dn,)),
            dma((schunks,)),
            dma,
        ],
        compiler_params=pltpu.CompilerParams(
            collective_id=0, has_side_effects=True, vmem_limit_bytes=56 * 1024 * 1024
        ),
        name="front",
    )(ts, tmask, tgain.reshape(1, feats), tproj, flat, gain1, sproj, smask)
    fixed = lambda shape: pl.BlockSpec(shape, lambda i: (0,) * len(shape))
    grad_embed, grad_states = pl.pallas_call(
        back,
        grid=(schunks,),
        out_shape=(
            jax.ShapeDtypeStruct((queries, embed), F32),
            jax.ShapeDtypeStruct((total, ds), BF16),
        ),
        in_specs=[
            fixed((dn * passages, embed)),
            fixed((queries, embed)),
            fixed((queries, 1)),
            fixed((queries, qlen)),
            fixed((1, ds)),
            fixed((ds, embed)),
            pl.BlockSpec((tokens, ds), lambda i: (i, 0)),
            pl.BlockSpec((tokens, embed), lambda i: (i, 0)),
        ],
        out_specs=(fixed((queries, embed)), pl.BlockSpec((tokens, ds), lambda i: (i, 0))),
        scratch_shapes=[pltpu.VMEM((queries, embed), F32)],
        compiler_params=pltpu.CompilerParams(vmem_limit_bytes=40 * 1024 * 1024),
        name="back",
    )(temb.reshape(dn * passages, embed), raw, positive.reshape(queries, 1), smask, gain1, sproj, flat, h)
    return grad_embed, grad_states.reshape(queries, qlen, ds)


def solution(mesh):
    in_specs = (
        P("dp", None, "mp"),
        P("mp"),
        P("mp", None),
        P("dp", None),
        P(("dp", "mp"), None, None),
        P(),
        P(),
        P(("dp", "mp"), None),
        P(("dp", "mp")),
    )
    out_specs = (P(("dp", "mp"), None), P(("dp", "mp"), None, None))
    body = functools.partial(shards, mesh.shape["dp"], mesh.shape["mp"])
    return jax.shard_map(body, mesh=mesh, in_specs=in_specs, out_specs=out_specs, check_vma=False)
```

```python
import functools

import jax
import jax.numpy as jnp
from jax import lax
from jax.experimental import pallas as pl
from jax.experimental.pallas import tpu as pltpu
from jax.sharding import PartitionSpec as P

MESH = pl.DeviceIdType.MESH
F32 = jnp.float32
BF16 = jnp.bfloat16
GROUPS = 4
QC = 4
ROOT = 0.7978845608028654
CUBE = 0.044715
NT = (((1,), (1,)), ((), ()))


def spread(live, chunk, tokens):
    queries, length = live.shape
    wide = jnp.concatenate([live] * (tokens // length), axis=1)
    row = lax.broadcasted_iota(jnp.int32, (queries, tokens), 0)
    col = lax.broadcasted_iota(jnp.int32, (queries, tokens), 1)
    return jnp.where(row == chunk * (tokens // length) + col // length, wide, 0.0)


def front(
    dn, n, ts, tmask, tgain, tproj, ss, sgain, sproj, smask, pos,
    embed_out, grad_out, h_out,
    tx, tp, sx, sp, sq, sqr, tpool, pf, pb, pr, te, hbuf, raw_out,
    sem_tx, sem_in, sq_send, sq_recv, rs_send, rs_recv, ag_send, ag_recv, dp_send, dp_recv, fw_send, fw_recv, h_sem,
):
    passages, length, feats = tx.shape
    width = n * feats
    rows = passages // n
    embed = tp.shape[1]
    chunks = passages // 8
    tokens = QC * smask.shape[1]
    schunks = sx.shape[0] // tokens
    me_d, me_m = lax.axis_index("dp"), lax.axis_index("mp")

    def mp_peer(o):
        return (me_d, lax.rem(me_m + o, n))

    def dp_peer(o):
        return (lax.rem(me_d + o, dn), me_m)

    def load(c):
        part = pl.ds(c * 8, 8)
        return pltpu.make_async_copy(ts.at[part], tx.at[part], sem_tx.at[c])

    others = [
        pltpu.make_async_copy(ss, sx, sem_in.at[0]),
        pltpu.make_async_copy(sproj, sp, sem_in.at[1]),
        pltpu.make_async_copy(tproj, tp, sem_in.at[2]),
    ]
    for c in range(chunks):
        load(c).start()
    for copy in others:
        copy.start()
    barrier = pltpu.get_barrier_semaphore()
    for o in range(1, n):
        pl.semaphore_signal(barrier, inc=1, device_id=mp_peer(o), device_id_type=MESH)
    for o in range(1, dn):
        pl.semaphore_signal(barrier, inc=1, device_id=dp_peer(o), device_id_type=MESH)

    def remote(src, dst, send, recv, peer):
        return pltpu.make_async_remote_copy(
            src_ref=src, dst_ref=dst, send_sem=send, recv_sem=recv, device_id=peer, device_id_type=MESH
        )

    ones = jnp.ones((16, 128), BF16)
    row8 = lax.broadcasted_iota(jnp.int32, (8, length), 0)
    per = chunks // GROUPS
    sq_copies = []
    for g in range(GROUPS):

        def squares(i, carry):
            c = g * per + i
            load(c).wait()
            held = jnp.zeros((8, length), F32)
            for j in range(8):
                total = None
                for k in range(feats // 128):
                    x = tx[c * 8 + j, :, k * 128 : (k + 1) * 128].astype(F32)
                    total = x * x if total is None else total + x * x
                line = lax.dot_general(ones, total.astype(BF16), NT, preferred_element_type=F32)
                held = jnp.where(row8 == j, line[:8], held)
            sq[c] = held
            return carry

        lax.fori_loop(0, per, squares, 0)
        if g == 0:
            pl.semaphore_wait(barrier, n + dn - 2)
        part = pl.ds(g * per, per)
        for o in range(1, n):
            copy = remote(sq.at[part], sqr.at[o, part], sq_send.at[o, g], sq_recv.at[o, g], mp_peer(o))
            copy.start()
            sq_copies.append(copy)

    row16 = lax.rem(lax.broadcasted_iota(jnp.int32, (16, length), 0), 8)
    for g in range(GROUPS):
        for o in range(1, n):
            sq_copies[g * (n - 1) + o - 1].wait_recv()

        def pool(i, carry):
            c = g * per + i
            total = sq[c]
            for o in range(1, n):
                total = total + sqr[o, c]
            part = pl.ds(pl.multiple_of(c * 8, 8), 8)
            weight = tmask[part, :].astype(F32) * lax.rsqrt(total / width + 1e-06)
            high = weight.astype(BF16).astype(F32)
            both = jnp.concatenate([high, weight - high], axis=0)
            left = jnp.concatenate([jnp.where(row16 == j, both, 0.0) for j in range(8)], axis=1).astype(BF16)
            sums = jnp.dot(left, tx[pl.ds(c * 8, 8)].reshape(8 * length, feats), preferred_element_type=F32)
            tpool[part, :] = (sums[:8] + sums[8:]) * tgain[...].reshape(1, feats)
            return carry

        lax.fori_loop(0, per, pool, 0)

    others[2].wait()
    partial = jnp.dot(tpool[...].astype(BF16), tp[...], preferred_element_type=F32)
    for j in range(n):
        block = partial[j * rows : (j + 1) * rows]
        pf[j] = block
        pb[j] = block.astype(BF16)
    rs_copies = []
    for o in range(1, n):
        copy = remote(pb.at[lax.rem(me_m + o, n)], pr.at[o], rs_send.at[o], rs_recv.at[o], mp_peer(o))
        copy.start()
        rs_copies.append(copy)

    live = smask[...].astype(F32)
    raw_out[...] = jnp.zeros_like(raw_out)
    others[0].wait()
    others[1].wait()

    def keep(i):
        part = pl.ds(pl.multiple_of(i * tokens, tokens), tokens)
        return pltpu.make_async_copy(hbuf.at[part], h_out.at[part], h_sem.at[i])

    def student(i, carry):
        part = pl.ds(pl.multiple_of(i * tokens, tokens), tokens)
        x = sx[part, :].astype(F32)
        scale = lax.rsqrt(jnp.mean(x * x, axis=-1, keepdims=True) + 1e-06)
        normed = (x * scale * sgain[...].reshape(1, sx.shape[1])).astype(BF16)
        picks = spread(live, i, tokens).astype(BF16)
        for k in range(embed // 256):
            cols = slice(k * 256, (k + 1) * 256)
            u = jnp.dot(normed, sp[:, cols], preferred_element_type=F32)
            uu = u * u
            th = jnp.tanh(u * (ROOT + (ROOT * CUBE) * uu))
            half = 0.5 + 0.5 * th
            act = u * half
            slope = half + act * (1.0 - th) * (ROOT + (3.0 * ROOT * CUBE) * uu)
            hbuf[part, cols] = slope.astype(BF16)
            raw_out[:, cols] += jnp.dot(picks, act.astype(BF16), preferred_element_type=F32)
        keep(i).start()
        return carry

    first, second, third = schunks // 4, 3 * schunks // 8, 7 * schunks // 8
    lax.fori_loop(0, first, student, 0)

    for copy in rs_copies:
        copy.wait_recv()
    summed = pf[me_m]
    for o in range(1, n):
        summed = summed + pr[o].astype(F32)
    unit = summed * lax.rsqrt(jnp.mean(summed * summed, axis=-1, keepdims=True) + 1e-06) * (embed ** -0.5)
    te[me_d, me_m] = unit.astype(BF16)
    ag_copies = []
    for o in range(1, n):
        copy = remote(te.at[me_d, me_m], te.at[me_d, me_m], ag_send.at[o], ag_recv.at[o], mp_peer(o))
        copy.start()
        ag_copies.append(copy)

    lax.fori_loop(first, second, student, 0)

    for copy in ag_copies:
        copy.wait_recv()
    dp_copies = []
    half = n // 2
    core = lax.rem(me_m, 2)
    mine = pl.ds(core * half, half)
    partner = (me_d, me_m + 1 - 2 * core)
    for o in range(1, dn):
        copy = remote(te.at[me_d, mine], te.at[me_d, mine], dp_send.at[o], dp_recv.at[o], dp_peer(o))
        copy.start()
        dp_copies.append(copy)

    lax.fori_loop(second, third, student, 0)

    fw_copies = []
    for o in range(1, dn):
        dp_copies[o - 1].wait_recv()
        came = te.at[lax.rem(me_d + dn - o, dn), mine]
        copy = remote(came, came, fw_send.at[o], fw_recv.at[o], partner)
        copy.start()
        fw_copies.append(copy)

    lax.fori_loop(third, schunks, student, 0)

    raw = raw_out[...]
    queries = raw.shape[0]
    scale = lax.rsqrt(jnp.mean(raw * raw, axis=-1, keepdims=True) + 1e-06)
    unit = scale * (embed ** -0.5)
    sround = (raw * unit).astype(BF16)
    total = dn * passages
    lines = lax.broadcasted_iota(jnp.int32, (total, queries), 0)
    picker = jnp.transpose(jnp.where(pos[...].reshape(1, queries) == lines, 1.0, 0.0)).astype(BF16)

    for copy in fw_copies:
        copy.wait_recv()
    table = te[...].reshape(total, embed)
    tpos = jnp.dot(picker, table, preferred_element_type=F32).astype(BF16)
    both = jnp.concatenate([tpos, sround], axis=0)
    logits = lax.dot_general(both, table, NT, preferred_element_type=F32)
    texp = jnp.exp(10.0 * logits[:queries])
    sexp = jnp.exp(20.0 * logits[queries:])
    diff = sexp / jnp.sum(sexp, axis=1, keepdims=True) - texp / jnp.sum(texp, axis=1, keepdims=True)
    ge = 20.0 * jnp.dot(diff.astype(BF16), table, preferred_element_type=F32)
    embed_out[...] = ge
    inner = jnp.mean(raw * ge, axis=-1, keepdims=True)
    grad_out[...] = unit * (ge - raw * (scale * scale * inner))
    for copy in sq_copies + rs_copies + ag_copies + dp_copies + fw_copies:
        copy.wait_send()
    for i in range(schunks):
        keep(i).wait()


def back(grad, smask, sgain, sproj, ss, h, states_out):
    step = pl.program_id(0)
    tokens = ss.shape[0]
    picks = jnp.transpose(spread(smask[...].astype(F32), step, tokens)).astype(BF16)
    wide = jnp.dot(picks, grad[...].astype(BF16), preferred_element_type=F32)
    du = (h[...].astype(F32) * wide).astype(BF16)
    dn = lax.dot_general(du, sproj[...], NT, preferred_element_type=F32)
    gy = dn.astype(BF16).astype(F32) * sgain[...].reshape(1, ss.shape[1])
    x = ss[...].astype(F32)
    scale = lax.rsqrt(jnp.mean(x * x, axis=-1, keepdims=True) + 1e-06)
    inner = jnp.mean(x * gy, axis=-1, keepdims=True)
    states_out[...] = (scale * gy - x * (scale * scale * scale * inner)).astype(BF16)


def shards(dn, n, ts, tgain, tproj, tmask, ss, sgain, sproj, smask, positive):
    passages, length, feats = ts.shape
    embed = tproj.shape[1]
    queries, qlen, ds = ss.shape
    rows = passages // n
    total = queries * qlen
    tokens = QC * qlen
    schunks = total // tokens
    chunks = passages // 8
    flat = ss.reshape(total, ds)
    anyspace = pl.BlockSpec(memory_space=pl.ANY)
    vmem = pl.BlockSpec(memory_space=pltpu.VMEM)
    dma = pltpu.SemaphoreType.DMA
    grad_embed, grad, h = pl.pallas_call(
        functools.partial(front, dn, n),
        out_shape=(
            jax.ShapeDtypeStruct((queries, embed), F32),
            jax.ShapeDtypeStruct((queries, embed), F32),
            jax.ShapeDtypeStruct((total, embed), BF16),
        ),
        in_specs=[anyspace, vmem, vmem, anyspace, anyspace, vmem, anyspace, vmem, vmem],
        out_specs=(vmem, vmem, anyspace),
        scratch_shapes=[
            pltpu.VMEM((passages, length, feats), BF16),
            pltpu.VMEM((feats, embed), BF16),
            pltpu.VMEM((total, ds), BF16),
            pltpu.VMEM((ds, embed), BF16),
            pltpu.VMEM((chunks, 8, length), F32),
            pltpu.VMEM((n, chunks, 8, length), F32),
            pltpu.VMEM((passages, feats), F32),
            pltpu.VMEM((n, rows, embed), F32),
            pltpu.VMEM((n, rows, embed), BF16),
            pltpu.VMEM((n, rows, embed), BF16),
            pltpu.VMEM((dn, n, rows, embed), BF16),
            pltpu.VMEM((total, embed), BF16),
            pltpu.VMEM((queries, embed), F32),
            dma((chunks,)),
            dma((3,)),
            dma((n, GROUPS)),
            dma((n, GROUPS)),
            dma((n,)),
            dma((n,)),
            dma((n,)),
            dma((n,)),
            dma((dn,)),
            dma((dn,)),
            dma((dn,)),
            dma((dn,)),
            dma((schunks,)),
        ],
        compiler_params=pltpu.CompilerParams(
            collective_id=0, has_side_effects=True, vmem_limit_bytes=56 * 1024 * 1024
        ),
        name="front",
    )(ts, tmask, tgain, tproj, flat, sgain, sproj, smask, positive)
    fixed = lambda shape: pl.BlockSpec(shape, lambda i: (0,) * len(shape))
    grad_states = pl.pallas_call(
        back,
        grid=(schunks,),
        out_shape=jax.ShapeDtypeStruct((total, ds), BF16),
        in_specs=[
            fixed((queries, embed)),
            fixed((queries, qlen)),
            fixed((ds,)),
            fixed((ds, embed)),
            pl.BlockSpec((tokens, ds), lambda i: (i, 0)),
            pl.BlockSpec((tokens, embed), lambda i: (i, 0)),
        ],
        out_specs=pl.BlockSpec((tokens, ds), lambda i: (i, 0)),
        compiler_params=pltpu.CompilerParams(vmem_limit_bytes=62 * 1024 * 1024),
        name="back",
    )(grad, smask, sgain, sproj, flat, h)
    return grad_embed, grad_states.reshape(queries, qlen, ds)


def solution(mesh):
    in_specs = (
        P("dp", None, "mp"),
        P("mp"),
        P("mp", None),
        P("dp", None),
        P(("dp", "mp"), None, None),
        P(),
        P(),
        P(("dp", "mp"), None),
        P(("dp", "mp")),
    )
    out_specs = (P(("dp", "mp"), None), P(("dp", "mp"), None, None))
    body = functools.partial(shards, mesh.shape["dp"], mesh.shape["mp"])
    return jax.shard_map(body, mesh=mesh, in_specs=in_specs, out_specs=out_specs, check_vma=False)
```

```python
import functools

import jax
import jax.numpy as jnp
from jax import lax
from jax.experimental import pallas as pl
from jax.experimental.pallas import tpu as pltpu
from jax.sharding import PartitionSpec as P

MESH = pl.DeviceIdType.MESH
F32 = jnp.float32
BF16 = jnp.bfloat16
GROUPS = 4
QC = 4
ROOT = 0.7978845608028654
CUBE = 0.044715
NT = (((1,), (1,)), ((), ()))


def spread(live, chunk, tokens):
    queries, length = live.shape
    wide = jnp.concatenate([live] * (tokens // length), axis=1)
    row = lax.broadcasted_iota(jnp.int32, (queries, tokens), 0)
    col = lax.broadcasted_iota(jnp.int32, (queries, tokens), 1)
    return jnp.where(row == chunk * (tokens // length) + col // length, wide, 0.0)


def front(
    dn, n, ts, tmask, tgain, tproj, ss, sgain, sproj, smask, pos,
    embed_out, grad_out, h_out,
    tx, tp, sx, sp, sq, sqr, tpool, pf, pb, pr, te, hbuf, raw_out,
    sem_tx, sem_in, sq_send, sq_recv, rs_send, rs_recv, ag_send, ag_recv, dp_send, dp_recv, fw_send, fw_recv, h_sem,
):
    passages, length, feats = tx.shape
    width = n * feats
    rows = passages // n
    embed = tp.shape[1]
    chunks = passages // 8
    tokens = QC * smask.shape[1]
    schunks = sx.shape[0] // tokens
    me_d, me_m = lax.axis_index("dp"), lax.axis_index("mp")

    def mp_peer(o):
        return (me_d, lax.rem(me_m + o, n))

    def dp_peer(o):
        return (lax.rem(me_d + o, dn), me_m)

    def load(c):
        part = pl.ds(c * 8, 8)
        return pltpu.make_async_copy(ts.at[part], tx.at[part], sem_tx.at[c])

    others = [
        pltpu.make_async_copy(ss, sx, sem_in.at[0]),
        pltpu.make_async_copy(sproj, sp, sem_in.at[1]),
        pltpu.make_async_copy(tproj, tp, sem_in.at[2]),
    ]
    ahead = min(4, chunks)
    for c in range(ahead):
        load(c).start()
    barrier = pltpu.get_barrier_semaphore()
    for o in range(1, n):
        pl.semaphore_signal(barrier, inc=1, device_id=mp_peer(o), device_id_type=MESH)
    for o in range(1, dn):
        pl.semaphore_signal(barrier, inc=1, device_id=dp_peer(o), device_id_type=MESH)

    def remote(src, dst, send, recv, peer):
        return pltpu.make_async_remote_copy(
            src_ref=src, dst_ref=dst, send_sem=send, recv_sem=recv, device_id=peer, device_id_type=MESH
        )

    ones = jnp.ones((16, 128), BF16)
    row8 = lax.broadcasted_iota(jnp.int32, (8, length), 0)
    per = chunks // GROUPS
    sq_copies = []
    for g in range(GROUPS):

        def squares(i, carry):
            c = g * per + i
            load(c).wait()

            @pl.when(c + ahead < chunks)
            def _():
                load(c + ahead).start()

            held = jnp.zeros((8, length), F32)
            for j in range(8):
                total = None
                for k in range(feats // 128):
                    x = tx[c * 8 + j, :, k * 128 : (k + 1) * 128].astype(F32)
                    total = x * x if total is None else total + x * x
                line = lax.dot_general(ones, total.astype(BF16), NT, preferred_element_type=F32)
                held = jnp.where(row8 == j, line[:8], held)
            sq[c] = held
            return carry

        lax.fori_loop(0, per, squares, 0)
        if g == 0:
            pl.semaphore_wait(barrier, n + dn - 2)
        if g == GROUPS // 2:
            for copy in others:
                copy.start()
        part = pl.ds(g * per, per)
        for o in range(1, n):
            copy = remote(sq.at[part], sqr.at[o, part], sq_send.at[o, g], sq_recv.at[o, g], mp_peer(o))
            copy.start()
            sq_copies.append(copy)

    row16 = lax.rem(lax.broadcasted_iota(jnp.int32, (16, length), 0), 8)
    for g in range(GROUPS):
        for o in range(1, n):
            sq_copies[g * (n - 1) + o - 1].wait_recv()

        def pool(i, carry):
            c = g * per + i
            total = sq[c]
            for o in range(1, n):
                total = total + sqr[o, c]
            part = pl.ds(pl.multiple_of(c * 8, 8), 8)
            weight = tmask[part, :].astype(F32) * lax.rsqrt(total / width + 1e-06)
            high = weight.astype(BF16).astype(F32)
            both = jnp.concatenate([high, weight - high], axis=0)
            left = jnp.concatenate([jnp.where(row16 == j, both, 0.0) for j in range(8)], axis=1).astype(BF16)
            sums = jnp.dot(left, tx[pl.ds(c * 8, 8)].reshape(8 * length, feats), preferred_element_type=F32)
            tpool[part, :] = (sums[:8] + sums[8:]) * tgain[...].reshape(1, feats)
            return carry

        lax.fori_loop(0, per, pool, 0)

    others[2].wait()
    partial = jnp.dot(tpool[...].astype(BF16), tp[...], preferred_element_type=F32)
    for j in range(n):
        block = partial[j * rows : (j + 1) * rows]
        pf[j] = block
        pb[j] = block.astype(BF16)
    rs_copies = []
    for o in range(1, n):
        copy = remote(pb.at[lax.rem(me_m + o, n)], pr.at[o], rs_send.at[o], rs_recv.at[o], mp_peer(o))
        copy.start()
        rs_copies.append(copy)

    live = smask[...].astype(F32)
    raw_out[...] = jnp.zeros_like(raw_out)
    others[0].wait()
    others[1].wait()

    def keep(i):
        part = pl.ds(pl.multiple_of(i * tokens, tokens), tokens)
        return pltpu.make_async_copy(hbuf.at[part], h_out.at[part], h_sem.at[i])

    def student(i, carry):
        part = pl.ds(pl.multiple_of(i * tokens, tokens), tokens)
        x = sx[part, :].astype(F32)
        scale = lax.rsqrt(jnp.mean(x * x, axis=-1, keepdims=True) + 1e-06)
        normed = (x * scale * sgain[...].reshape(1, sx.shape[1])).astype(BF16)
        picks = spread(live, i, tokens).astype(BF16)
        for k in range(embed // 256):
            cols = slice(k * 256, (k + 1) * 256)
            u = jnp.dot(normed, sp[:, cols], preferred_element_type=F32)
            uu = u * u
            th = jnp.tanh(u * (ROOT + (ROOT * CUBE) * uu))
            half = 0.5 + 0.5 * th
            act = u * half
            slope = half + act * (1.0 - th) * (ROOT + (3.0 * ROOT * CUBE) * uu)
            hbuf[part, cols] = slope.astype(BF16)
            raw_out[:, cols] += jnp.dot(picks, act.astype(BF16), preferred_element_type=F32)
        keep(i).start()
        return carry

    first, second, third = schunks // 4, 3 * schunks // 8, 7 * schunks // 8
    lax.fori_loop(0, first, student, 0)

    for copy in rs_copies:
        copy.wait_recv()
    summed = pf[me_m]
    for o in range(1, n):
        summed = summed + pr[o].astype(F32)
    unit = summed * lax.rsqrt(jnp.mean(summed * summed, axis=-1, keepdims=True) + 1e-06) * (embed ** -0.5)
    te[me_d, me_m] = unit.astype(BF16)
    ag_copies = []
    for o in range(1, n):
        copy = remote(te.at[me_d, me_m], te.at[me_d, me_m], ag_send.at[o], ag_recv.at[o], mp_peer(o))
        copy.start()
        ag_copies.append(copy)

    lax.fori_loop(first, second, student, 0)

    for copy in ag_copies:
        copy.wait_recv()
    dp_copies = []
    half = n // 2
    core = lax.rem(me_m, 2)
    mine = pl.ds(core * half, half)
    partner = (me_d, me_m + 1 - 2 * core)
    for o in range(1, dn):
        copy = remote(te.at[me_d, mine], te.at[me_d, mine], dp_send.at[o], dp_recv.at[o], dp_peer(o))
        copy.start()
        dp_copies.append(copy)

    lax.fori_loop(second, third, student, 0)

    fw_copies = []
    for o in range(1, dn):
        dp_copies[o - 1].wait_recv()
        came = te.at[lax.rem(me_d + dn - o, dn), mine]
        copy = remote(came, came, fw_send.at[o], fw_recv.at[o], partner)
        copy.start()
        fw_copies.append(copy)

    lax.fori_loop(third, schunks, student, 0)

    raw = raw_out[...]
    queries = raw.shape[0]
    scale = lax.rsqrt(jnp.mean(raw * raw, axis=-1, keepdims=True) + 1e-06)
    unit = scale * (embed ** -0.5)
    sround = (raw * unit).astype(BF16)
    total = dn * passages
    lines = lax.broadcasted_iota(jnp.int32, (total, queries), 0)
    picker = jnp.transpose(jnp.where(pos[...].reshape(1, queries) == lines, 1.0, 0.0)).astype(BF16)

    for copy in fw_copies:
        copy.wait_recv()
    table = te[...].reshape(total, embed)
    tpos = jnp.dot(picker, table, preferred_element_type=F32).astype(BF16)
    both = jnp.concatenate([tpos, sround], axis=0)
    logits = lax.dot_general(both, table, NT, preferred_element_type=F32)
    texp = jnp.exp(10.0 * logits[:queries])
    sexp = jnp.exp(20.0 * logits[queries:])
    diff = sexp / jnp.sum(sexp, axis=1, keepdims=True) - texp / jnp.sum(texp, axis=1, keepdims=True)
    ge = 20.0 * jnp.dot(diff.astype(BF16), table, preferred_element_type=F32)
    embed_out[...] = ge
    inner = jnp.mean(raw * ge, axis=-1, keepdims=True)
    grad_out[...] = unit * (ge - raw * (scale * scale * inner))
    for copy in sq_copies + rs_copies + ag_copies + dp_copies + fw_copies:
        copy.wait_send()
    for i in range(schunks):
        keep(i).wait()


def back(ge, grad, smask, sgain, sproj, ss, h, embed_out, states_out):
    step = pl.program_id(0)
    tokens = ss.shape[0]

    @pl.when(step == 0)
    def _():
        embed_out[...] = ge[...]

    picks = jnp.transpose(spread(smask[...].astype(F32), step, tokens)).astype(BF16)
    wide = jnp.dot(picks, grad[...].astype(BF16), preferred_element_type=F32)
    du = (h[...].astype(F32) * wide).astype(BF16)
    dn = lax.dot_general(du, sproj[...], NT, preferred_element_type=F32)
    gy = dn.astype(BF16).astype(F32) * sgain[...].reshape(1, ss.shape[1])
    x = ss[...].astype(F32)
    scale = lax.rsqrt(jnp.mean(x * x, axis=-1, keepdims=True) + 1e-06)
    inner = jnp.mean(x * gy, axis=-1, keepdims=True)
    states_out[...] = (scale * gy - x * (scale * scale * scale * inner)).astype(BF16)


def shards(dn, n, ts, tgain, tproj, tmask, ss, sgain, sproj, smask, positive):
    passages, length, feats = ts.shape
    embed = tproj.shape[1]
    queries, qlen, ds = ss.shape
    rows = passages // n
    total = queries * qlen
    tokens = QC * qlen
    schunks = total // tokens
    chunks = passages // 8
    flat = ss.reshape(total, ds)
    anyspace = pl.BlockSpec(memory_space=pl.ANY)
    vmem = pl.BlockSpec(memory_space=pltpu.VMEM)
    dma = pltpu.SemaphoreType.DMA
    ge, grad, h = pl.pallas_call(
        functools.partial(front, dn, n),
        out_shape=(
            jax.ShapeDtypeStruct((queries, embed), F32),
            jax.ShapeDtypeStruct((queries, embed), F32),
            jax.ShapeDtypeStruct((total, embed), BF16),
        ),
        in_specs=[anyspace, vmem, vmem, anyspace, anyspace, vmem, anyspace, vmem, vmem],
        out_specs=(vmem, vmem, anyspace),
        scratch_shapes=[
            pltpu.VMEM((passages, length, feats), BF16),
            pltpu.VMEM((feats, embed), BF16),
            pltpu.VMEM((total, ds), BF16),
            pltpu.VMEM((ds, embed), BF16),
            pltpu.VMEM((chunks, 8, length), F32),
            pltpu.VMEM((n, chunks, 8, length), F32),
            pltpu.VMEM((passages, feats), F32),
            pltpu.VMEM((n, rows, embed), F32),
            pltpu.VMEM((n, rows, embed), BF16),
            pltpu.VMEM((n, rows, embed), BF16),
            pltpu.VMEM((dn, n, rows, embed), BF16),
            pltpu.VMEM((total, embed), BF16),
            pltpu.VMEM((queries, embed), F32),
            dma((chunks,)),
            dma((3,)),
            dma((n, GROUPS)),
            dma((n, GROUPS)),
            dma((n,)),
            dma((n,)),
            dma((n,)),
            dma((n,)),
            dma((dn,)),
            dma((dn,)),
            dma((dn,)),
            dma((dn,)),
            dma((schunks,)),
        ],
        compiler_params=pltpu.CompilerParams(
            collective_id=0, has_side_effects=True, vmem_limit_bytes=56 * 1024 * 1024
        ),
        name="front",
    )(ts, tmask, tgain, tproj, flat, sgain, sproj, smask, positive)
    fixed = lambda shape: pl.BlockSpec(shape, lambda i: (0,) * len(shape))
    grad_embed, grad_states = pl.pallas_call(
        back,
        grid=(schunks,),
        out_shape=(jax.ShapeDtypeStruct((queries, embed), F32), jax.ShapeDtypeStruct((total, ds), BF16)),
        in_specs=[
            fixed((queries, embed)),
            fixed((queries, embed)),
            fixed((queries, qlen)),
            fixed((ds,)),
            fixed((ds, embed)),
            pl.BlockSpec((tokens, ds), lambda i: (i, 0)),
            pl.BlockSpec((tokens, embed), lambda i: (i, 0)),
        ],
        out_specs=(fixed((queries, embed)), pl.BlockSpec((tokens, ds), lambda i: (i, 0))),
        compiler_params=pltpu.CompilerParams(vmem_limit_bytes=62 * 1024 * 1024),
        name="back",
    )(ge, grad, smask, sgain, sproj, flat, h)
    return grad_embed, grad_states.reshape(queries, qlen, ds)


def solution(mesh):
    in_specs = (
        P("dp", None, "mp"),
        P("mp"),
        P("mp", None),
        P("dp", None),
        P(("dp", "mp"), None, None),
        P(),
        P(),
        P(("dp", "mp"), None),
        P(("dp", "mp")),
    )
    out_specs = (P(("dp", "mp"), None), P(("dp", "mp"), None, None))
    body = functools.partial(shards, mesh.shape["dp"], mesh.shape["mp"])
    return jax.shard_map(body, mesh=mesh, in_specs=in_specs, out_specs=out_specs, check_vma=False)
```
